256 devices in a mesh: grp: 8 (over y, core), dom: 32 (over z, x).
Axes of the slice: x: 4, y: 4, z: 8, core: 2. Of those that a mesh axis runs over, the one named last changes fastest.
Arguments:
- element_state: float32 [56, 9, 163840], P(None, None, ('grp', 'dom')), may hold values from -6 to 6
- stiffness: float32 [3, 56, 56], replicated, may hold values from -0.75 to 0.75
- flux_local: float32 [4, 56, 56], replicated, may hold values from -0.75 to 0.75
- flux_remote: float32 [4, 56, 56], replicated, may hold values from -0.75 to 0.75
- star_matrix: float32 [3, 9, 9, 163840], P(None, None, None, ('grp', 'dom')), may hold values from -0.18 to 0.18
- face_local: float32 [4, 9, 9, 163840], P(None, None, None, ('grp', 'dom')), may hold values from -0.15 to 0.15
- face_remote: float32 [4, 9, 9, 163840], P(None, None, None, ('grp', 'dom')), may hold values from -0.15 to 0.15
- energy_weight: float32 [9, 163840], P(None, ('grp', 'dom')), may hold values from 0.5 to 18
- face_neighbour: int32 [4, 163840], P(None, ('grp', 'dom')), may hold values from 0 to 1151, as said below
- element_count: int32 [256], P(('grp', 'dom')), may hold values from 160 to 640, as said below
- send_count: int32 [256, 8], P(('grp', 'dom')), may hold values from 0 to 64, as said below
- send_element: int32 [256, 8, 64], P(('grp', 'dom')), may hold values from 0 to 639, as said below
- receiver_element: int32 [4096], P(('grp', 'dom')), may hold values from 0 to 639, as said below
- receiver_slot: int32 [4096], P(('grp', 'dom')), may hold values from 0 to 511, as said below
- receiver_weight: float32 [56, 4096], P(None, ('grp', 'dom')), may hold values from -0.75 to 0.75
Outputs:
- new_state: float32 [56, 9, 163840], P(None, None, ('grp', 'dom'))
- energy: float32 [8, 3], P('grp')
- traces: float32 [3, 9, 4096], P(None, None, ('grp', 'dom'))
The draws below stay inside these ranges and needn't reach their ends.
Inputs may be any that keep to these rules, and one draw needn't show every extreme that they name: The first element_count[p] slots of a partition are active. In every slab 4 partitions in a row along dom (cyclically) hold 640 active elements; the others hold from 160 to 320. `send_count`: every partition has exactly 64 in one of its first 6 slots. `send_element`: names active elements of the sending partition. `face_neighbour`: values below 640 name active elements of the partition itself. `receiver_element`: names an active element of the owning partition. `receiver_slot`: within each slab a permutation of the 512 rows.
All inputs are finite; a program needn't handle non-finite values.
Results may differ from the reference program's by a relative error of at most 0.0001.
Values sent between devices are 32-bit elements; how exact they have to be, the bound alone decides.
No kernel may reach another device: no remote copies, remote signals or barrier semaphores. Data moves between devices by JAX's collectives and lax.ppermute only.
A program may use at most 128 MiB of HBM per device.

```python
import jax
import jax.numpy as jnp
from jax import lax

BASIS_MODES = 56
QUANTITIES = 9
DIMENSIONS = 3
ELEM_FACES = 4
PEER_REACH = 3
TIME_STEPS = 3
HALO_CAP = 64
ELEM_PAD = 640
REC_DEV = 16
GROUPS = 8
GROUP_SIZE = 32
PARTITIONS = 256
PEER_SLOTS = 8
ELEMENTS = 163840
RECEIVERS = 4096


def partition_counts(key):
    base = jax.random.fold_in(key, 101)
    lighter = jax.random.randint(jax.random.fold_in(base, 1), (PARTITIONS,), ELEM_PAD // 4, ELEM_PAD // 2 + 1)
    window = jax.random.randint(jax.random.fold_in(base, 2), (GROUPS,), 0, GROUP_SIZE)
    numbers = jnp.arange(PARTITIONS, dtype=jnp.int32)
    position = (numbers % GROUP_SIZE - window[numbers // GROUP_SIZE]) % GROUP_SIZE
    return jnp.where(position < 4, ELEM_PAD, lighter).astype(jnp.int32)


def draw_element_count(key, part):
    return partition_counts(key)


def draw_send_count(key, part):
    counted = jax.random.randint(jax.random.fold_in(key, 201), (PARTITIONS, PEER_SLOTS), 0, HALO_CAP + 1)
    fullest = jax.random.randint(jax.random.fold_in(key, 202), (PARTITIONS, 1), 0, 2 * PEER_REACH)
    slots_row = jnp.arange(PEER_SLOTS, dtype=jnp.int32)[None, :]
    return jnp.where(slots_row == fullest, HALO_CAP, counted).astype(jnp.int32)


def draw_send_element(key, part):
    counts = partition_counts(key)
    return jax.random.randint(jax.random.fold_in(key, 301), (PARTITIONS, PEER_SLOTS, HALO_CAP), 0, counts[:, None, None]).astype(jnp.int32)


def draw_face_neighbour(key, part):
    counts = partition_counts(key)
    limits = jnp.repeat(counts, ELEM_PAD, total_repeat_length=ELEMENTS)[None, :]
    own_side = jax.random.randint(jax.random.fold_in(key, 401), (ELEM_FACES, ELEMENTS), 0, limits)
    far_side = ELEM_PAD + jax.random.randint(jax.random.fold_in(key, 402), (ELEM_FACES, ELEMENTS), 0, PEER_SLOTS * HALO_CAP)
    chosen = jax.random.randint(jax.random.fold_in(key, 403), (ELEM_FACES, ELEMENTS), 0, 4) == 0
    return jnp.where(chosen, far_side, own_side).astype(jnp.int32)


def draw_receiver_element(key, part):
    counts = partition_counts(key)
    limits = jnp.repeat(counts, REC_DEV, total_repeat_length=RECEIVERS)
    return jax.random.randint(jax.random.fold_in(key, 501), (RECEIVERS,), 0, limits).astype(jnp.int32)


def draw_receiver_slot(key, part):
    group_keys = jax.random.split(jax.random.fold_in(key, 601), GROUPS)
    orders = jax.vmap(lambda group_key: jax.random.permutation(group_key, GROUP_SIZE * REC_DEV))(group_keys)
    return orders.reshape(-1).astype(jnp.int32)


def draw_energy_weight(key, part):
    uniform_part = jax.random.uniform(jax.random.fold_in(key, 701), (QUANTITIES, ELEMENTS), jnp.float32)
    position = (jnp.arange(ELEMENTS, dtype=jnp.int32) // ELEM_PAD % GROUP_SIZE).astype(jnp.float32)
    rising = 1.0 + 2.0 * position / (GROUP_SIZE - 1)
    return (jnp.exp(jnp.log(0.5) + uniform_part * jnp.log(4.0)) * rising).astype(jnp.float32)


def level_of(key, shape, cuts, low, largest):
    gain = 1.0
    for axis_at, blocks in cuts:
        draws = jax.random.uniform(jax.random.fold_in(jax.random.fold_in(key, 6), axis_at), (blocks,), jnp.float32, low / len(cuts), largest / len(cuts))
        gain = gain * jnp.repeat(jnp.exp(draws), shape[axis_at] // blocks).reshape((-1,) + (1,) * (len(shape) - 1 - axis_at))
    return gain


def normal_values(rng, shape, deviation, bound, cuts=(), kind=jnp.bfloat16):
    result = deviation * jax.random.normal(rng, shape, jnp.float32)
    if cuts:
        result = result * level_of(rng, shape, cuts, -0.22, 0.18)
    return jnp.clip(result, -bound, bound).astype(kind)


def setup_inputs(seed: int = 0) -> dict:
    arg_keys = jax.random.split(jax.random.key(seed), 16)
    element_state = normal_values(arg_keys[0], (BASIS_MODES, QUANTITIES, ELEMENTS), 1.0, 6.0, ((2, 256),), jnp.float32)
    stiffness = normal_values(arg_keys[1], (DIMENSIONS, BASIS_MODES, BASIS_MODES), BASIS_MODES ** -0.5, 0.75, (), jnp.float32)
    flux_local = normal_values(arg_keys[2], (ELEM_FACES, BASIS_MODES, BASIS_MODES), BASIS_MODES ** -0.5, 0.75, (), jnp.float32)
    flux_remote = normal_values(arg_keys[3], (ELEM_FACES, BASIS_MODES, BASIS_MODES), BASIS_MODES ** -0.5, 0.75, (), jnp.float32)
    star_matrix = normal_values(arg_keys[4], (DIMENSIONS, QUANTITIES, QUANTITIES, ELEMENTS), 0.03, 0.18, ((3, 256),), jnp.float32)
    face_local = normal_values(arg_keys[5], (ELEM_FACES, QUANTITIES, QUANTITIES, ELEMENTS), 0.025, 0.15, ((3, 256),), jnp.float32)
    face_remote = normal_values(arg_keys[6], (ELEM_FACES, QUANTITIES, QUANTITIES, ELEMENTS), 0.025, 0.15, ((3, 256),), jnp.float32)
    energy_weight = draw_energy_weight(jax.random.fold_in(arg_keys[15], 71), 0)
    face_neighbour = draw_face_neighbour(jax.random.fold_in(arg_keys[15], 71), 0)
    element_count = draw_element_count(jax.random.fold_in(arg_keys[15], 71), 0)
    send_count = draw_send_count(jax.random.fold_in(arg_keys[15], 71), 0)
    send_element = draw_send_element(jax.random.fold_in(arg_keys[15], 71), 0)
    receiver_element = draw_receiver_element(jax.random.fold_in(arg_keys[15], 71), 0)
    receiver_slot = draw_receiver_slot(jax.random.fold_in(arg_keys[15], 71), 0)
    receiver_weight = normal_values(arg_keys[14], (BASIS_MODES, RECEIVERS), BASIS_MODES ** -0.5, 0.75, ((1, 256),), jnp.float32)
    return dict(element_state=element_state, stiffness=stiffness, flux_local=flux_local, flux_remote=flux_remote, star_matrix=star_matrix, face_local=face_local, face_remote=face_remote, energy_weight=energy_weight, face_neighbour=face_neighbour, element_count=element_count, send_count=send_count, send_element=send_element, receiver_element=receiver_element, receiver_slot=receiver_slot, receiver_weight=receiver_weight)


highest = lax.Precision.HIGHEST


def modal(matrix, field):
    flat = field.reshape(field.shape[0], -1)
    product = jnp.dot(matrix, flat, precision=highest, preferred_element_type=jnp.float32)
    return product.reshape((matrix.shape[0],) + field.shape[1:])


def quantity_map(matrices, field):
    return jnp.einsum("pqe,bqe->bpe", matrices, field, precision=highest)


def per_partition(array):
    shaped = array.reshape(array.shape[:-1] + (PARTITIONS, ELEM_PAD))
    return jnp.moveaxis(shaped, -2, 0)


def slot_offset(slot_number):
    if slot_number < PEER_REACH:
        return slot_number + 1
    if slot_number < 2 * PEER_REACH:
        return PEER_REACH - 1 - slot_number
    if slot_number == 2 * PEER_REACH:
        return 1
    return -1


def reference(element_state, stiffness, flux_local, flux_remote, star_matrix, face_local, face_remote, energy_weight, face_neighbour, element_count, send_count, send_element, receiver_element, receiver_slot, receiver_weight):
    fields = per_partition(element_state)
    stars = per_partition(star_matrix)
    local_faces = per_partition(face_local)
    remote_faces = per_partition(face_remote)
    weights = per_partition(energy_weight)
    neighbours = per_partition(face_neighbour)
    receiver_rows = jnp.moveaxis(receiver_weight.reshape(BASIS_MODES, PARTITIONS, REC_DEV), 1, 0)
    receiver_cells = receiver_element.reshape(PARTITIONS, REC_DEV)
    numbers = jnp.arange(PARTITIONS, dtype=jnp.int32)
    group_of = numbers // GROUP_SIZE
    place_of = numbers % GROUP_SIZE
    source_list = []
    present_list = []
    for slot_number in range(PEER_SLOTS):
        offset = slot_offset(slot_number)
        if slot_number < 2 * PEER_REACH:
            source_list.append(group_of * GROUP_SIZE + (place_of - offset) % GROUP_SIZE)
            present_list.append(jnp.ones((PARTITIONS,), dtype=bool))
        else:
            other = group_of - offset
            present_list.append((other >= 0) & (other < GROUPS))
            source_list.append(jnp.clip(other, 0, GROUPS - 1) * GROUP_SIZE + place_of)
    sources = jnp.stack(source_list, 1).astype(jnp.int32)
    present = jnp.stack(present_list, 1)
    live_mask = jnp.arange(ELEM_PAD, dtype=jnp.int32)[None, :] < element_count[:, None]
    slot_live = jnp.arange(HALO_CAP, dtype=jnp.int32)[None, None, :] < send_count[:, :, None]
    denominator = GROUP_SIZE * ELEM_PAD * BASIS_MODES * QUANTITIES
    global_slot = ((jnp.arange(RECEIVERS, dtype=jnp.int32) // (GROUP_SIZE * REC_DEV)) * (GROUP_SIZE * REC_DEV) + receiver_slot).astype(jnp.int32)

    def pack(field, elements, live):
        taken = jnp.take(field, elements, axis=2)
        return jnp.where(live[None, None], taken, jnp.float32(0.0))

    def advance(fields):
        messages = jax.vmap(pack)(fields, send_element, slot_live)

        def update_one(items):
            field, star_here, local_here, remote_here, neighbour_here, source_here, present_here, live_here = items
            pieces = []
            for slot_number in range(PEER_SLOTS):
                sent = lax.dynamic_index_in_dim(messages, source_here[slot_number], 0, keepdims=False)[:, :, slot_number, :]
                pieces.append(jnp.where(present_here[slot_number], sent, jnp.float32(0.0)))
            halo = jnp.stack(pieces, 2).reshape(BASIS_MODES, QUANTITIES, PEER_SLOTS * HALO_CAP)
            extended = jnp.concatenate([field, halo], 2)
            change = jnp.zeros(field.shape, jnp.float32)
            for dimension in range(DIMENSIONS):
                change = change + quantity_map(star_here[dimension], modal(stiffness[dimension], field))
            for face_number in range(ELEM_FACES):
                change = change - quantity_map(local_here[face_number], modal(flux_local[face_number], field))
                nearby = jnp.take(extended, neighbour_here[face_number], axis=2)
                change = change - quantity_map(remote_here[face_number], modal(flux_remote[face_number], nearby))
            return jnp.where(live_here[None, None, :], field + change, field)

        return lax.map(update_one, (fields, stars, local_faces, remote_faces, neighbours, sources, present, live_mask))

    energies = []
    tables = []
    for time_step in range(TIME_STEPS):
        fields = advance(fields)
        squares = jnp.sum(fields * fields, axis=1)
        terms = 0.5 * jnp.sum(jnp.where(live_mask[:, None, :], weights * squares, jnp.float32(0.0)), axis=(1, 2))
        energies.append(terms.reshape(GROUPS, GROUP_SIZE).sum(1) / denominator)

        def sample(field, elements, rows_here):
            return jnp.einsum("br,bqr->qr", rows_here, jnp.take(field, elements, axis=2), precision=highest)

        values = jax.vmap(sample)(fields, receiver_cells, receiver_rows)
        flat = jnp.moveaxis(values, 0, 1).reshape(QUANTITIES, RECEIVERS)
        tables.append(jnp.zeros((QUANTITIES, RECEIVERS), jnp.float32).at[:, global_slot].set(flat))
    new_state = jnp.moveaxis(fields, 0, 2).reshape(BASIS_MODES, QUANTITIES, ELEMENTS)
    return new_state, jnp.stack(energies, 1), jnp.stack(tables, 0)
```

```python
import jax
import jax.numpy as jnp
from jax import lax
from jax.experimental import pallas as pl
from jax.experimental.pallas import tpu as pltpu
from jax.sharding import PartitionSpec as P

PEER_REACH = 3
TIME_STEPS = 3
GRP_DOM = ("grp", "dom")
LANES = 128
HALF = 64
SEND_ROWS = 256
F32 = jnp.float32
BF16 = jnp.bfloat16
highest = lax.Precision.HIGHEST


def two_parts(value):
    high = value.astype(BF16)
    low = (value - high.astype(F32)).astype(BF16)
    return high, low


def dot(a, b):
    return jnp.dot(a, b, preferred_element_type=F32)


def padded_k(matrices):
    rounded = lax.reduce_precision(matrices, 8, 7)
    high = rounded.astype(BF16)
    low = (matrices - rounded).astype(BF16)
    fill = jnp.zeros((matrices.shape[0], HALF - matrices.shape[1]), BF16)
    return jnp.concatenate([high, fill, high, fill, low, fill], 1)


def stack_columns(field, rhs_ref):
    basis = field.shape[0]
    high, low = two_parts(field)
    rhs_ref[0:basis, :] = high
    rhs_ref[HALF : HALF + basis, :] = low
    rhs_ref[2 * HALF : 2 * HALF + basis, :] = high


def clear_fill(rhs_ref, basis):
    for part in range(3):
        rhs_ref[part * HALF + basis : (part + 1) * HALF, :] = jnp.zeros(
            (HALF - basis, rhs_ref.shape[1]), BF16
        )


def apply_maps(tile, matrices, terms_ref, base, emit, quantities, basis):
    lanes = pl.ds(pl.multiple_of(tile * LANES, LANES), LANES)
    group = 3
    for first in range(0, quantities, group):
        rows = list(range(first, min(first + group, quantities)))
        total = [base(p, lanes) for p in rows]
        for n, (ref, at, slot) in enumerate(matrices):
            for q in range(quantities):
                term = terms_ref[slot, q * basis : (q + 1) * basis, lanes]
                for k, p in enumerate(rows):
                    total[k] = total[k] + ref[at, p, q : q + 1, lanes] * term
        for k, p in enumerate(rows):
            emit(p, lanes, total[k])


def pack(field, select_ref, weight_ref, message_refs, values_ref, quantities, basis):
    rows = quantities * basis
    high, low = two_parts(field)
    lane = lax.broadcasted_iota(jnp.int32, (SEND_ROWS, LANES), 1) < HALF
    tail = SEND_ROWS - (rows - SEND_ROWS)
    pairs = len(message_refs) // 2
    for pair in range(pairs + 1):
        chosen = select_ref[:, pair * LANES : (pair + 1) * LANES]
        picked = dot(high, chosen) + dot(low, chosen)
        if pair == pairs:
            for q in range(quantities):
                values_ref[q : q + 1, :] = jnp.sum(
                    picked[q * basis : (q + 1) * basis] * weight_ref[...], axis=0, keepdims=True
                )
        else:
            top = picked[:SEND_ROWS]
            bottom = jnp.concatenate([picked[SEND_ROWS:], jnp.zeros((tail, LANES), F32)], 0)
            message_refs[2 * pair][...] = jnp.where(lane, top, pltpu.roll(bottom, HALF, 1))
            message_refs[2 * pair + 1][...] = jnp.where(lane, pltpu.roll(top, HALF, 1), bottom)


def first_kernel(state_ref, select_ref, weight_ref, *outs):
    basis, quantities, _ = state_ref.shape
    field_ref, values_ref = outs[0], outs[-1]
    messages = outs[1:-1]
    for q in range(quantities):
        field_ref[q * basis : (q + 1) * basis, :] = state_ref[:, q, :]
    pack(field_ref[...], select_ref, weight_ref, messages, values_ref, quantities, basis)


def own_kernel(field_ref, matrix_ref, star_ref, local_ref, remote_ref, choose_ref, out_ref, terms_ref, rhs_ref):
    faces = remote_ref.shape[0]
    locals_ = star_ref.shape[0] + faces
    quantities = star_ref.shape[1]
    basis = field_ref.shape[0] // quantities
    width = field_ref.shape[1]
    clear_fill(rhs_ref, basis)

    def modal(q, carry):
        rows = pl.ds(pl.multiple_of(q * basis, 8), basis)
        stack_columns(field_ref[rows, :], rhs_ref)
        for n in range(locals_ + faces):
            terms_ref[n, rows, :] = dot(matrix_ref[n * basis : (n + 1) * basis, :], rhs_ref[...])
        return carry

    lax.fori_loop(0, quantities, modal, 0)

    def gather(f, carry):
        high, low = two_parts(terms_ref[locals_ + f])
        chosen = choose_ref[f]
        terms_ref[locals_ + f] = dot(high, chosen) + dot(low, chosen)
        return carry

    lax.fori_loop(0, faces, gather, 0)
    matrices = (
        [(star_ref, n, n) for n in range(star_ref.shape[0])]
        + [(local_ref, f, star_ref.shape[0] + f) for f in range(faces)]
        + [(remote_ref, f, locals_ + f) for f in range(faces)]
    )

    def tile_body(tile, carry):
        def base(p, lanes):
            return field_ref[p * basis : (p + 1) * basis, lanes]

        def emit(p, lanes, value):
            out_ref[p * basis : (p + 1) * basis, lanes] = value

        apply_maps(tile, matrices, terms_ref, base, emit, quantities, basis)
        return carry

    lax.fori_loop(0, width // LANES, tile_body, 0)


def halo_kernel(last, count_ref, field_ref, partial_ref, matrix_ref, remote_ref, choose_ref, energy_ref, select_ref, weight_ref, *rest):
    slots = 8
    halo_refs = rest[:slots]
    rest = rest[slots:]
    if last:
        state_ref, power_ref, values_ref = rest[:3]
        messages = ()
        scratch = rest[3:]
    else:
        state_ref, power_ref, values_ref = rest[0], rest[1], rest[2]
        messages = rest[3 : 3 + slots]
        scratch = rest[3 + slots :]
    columns_ref, flux_ref, terms_ref, rhs_ref, new_ref = scratch
    faces, quantities = remote_ref.shape[0], remote_ref.shape[1]
    basis = field_ref.shape[0] // quantities
    rows_all, width = field_ref.shape
    clear_fill(rhs_ref, basis)
    lane = lax.broadcasted_iota(jnp.int32, (SEND_ROWS, LANES), 1) < HALF
    for pair in range(slots // 2):
        a = halo_refs[2 * pair][...]
        b = halo_refs[2 * pair + 1][...]
        lanes = slice(pair * LANES, (pair + 1) * LANES)
        columns_ref[0:SEND_ROWS, lanes] = jnp.where(lane, a, pltpu.roll(b, HALF, 1))
        bottom = jnp.where(lane, pltpu.roll(a, HALF, 1), b)
        columns_ref[SEND_ROWS:, lanes] = bottom[: rows_all - SEND_ROWS]

    def modal(q, carry):
        rows = pl.ds(pl.multiple_of(q * basis, 8), basis)
        stack_columns(columns_ref[rows, :], rhs_ref)
        for f in range(faces):
            flux_ref[f, rows, :] = dot(matrix_ref[f * basis : (f + 1) * basis, :], rhs_ref[...])
        return carry

    lax.fori_loop(0, quantities, modal, 0)

    def gather(f, carry):
        high, low = two_parts(flux_ref[f])
        chosen = choose_ref[f]
        terms_ref[f] = dot(high, chosen) + dot(low, chosen)
        return carry

    lax.fori_loop(0, faces, gather, 0)
    matrices = [(remote_ref, f, f) for f in range(faces)]

    def tile_body(tile, power):
        lane_number = lax.broadcasted_iota(jnp.int32, (basis, LANES), 1) + tile * LANES
        live = lane_number < count_ref[0]
        totals = [power]

        def base(p, lanes):
            return partial_ref[p * basis : (p + 1) * basis, lanes]

        def emit(p, lanes, value):
            kept = jnp.where(live, value, field_ref[p * basis : (p + 1) * basis, lanes])
            new_ref[p * basis : (p + 1) * basis, lanes] = kept
            squares = jnp.where(live, kept * kept, 0.0) * energy_ref[p : p + 1, lanes]
            for block in range(basis // 8):
                totals[0] = totals[0] + squares[block * 8 : (block + 1) * 8]

        apply_maps(tile, matrices, terms_ref, base, emit, quantities, basis)
        return totals[0]

    power_ref[...] = lax.fori_loop(0, width // LANES, tile_body, jnp.zeros((8, LANES), F32))
    if last:
        for q in range(quantities):
            state_ref[:, q, :] = new_ref[q * basis : (q + 1) * basis, :]
        pack(new_ref[...], select_ref, weight_ref, messages, values_ref, quantities, basis)
    else:
        state_ref[...] = new_ref[...]
        pack(new_ref[...], select_ref, weight_ref, messages, values_ref, quantities, basis)


def vmem(count):
    return [pl.BlockSpec(memory_space=pltpu.VMEM)] * count


def per_device(
    element_state,
    stiffness,
    flux_local,
    flux_remote,
    star_matrix,
    face_local,
    face_remote,
    energy_weight,
    face_neighbour,
    element_count,
    send_count,
    send_element,
    receiver_element,
    receiver_slot,
    receiver_weight,
):
    basis, quantities, width = element_state.shape
    slots, capacity = send_element.shape[1:]
    faces = face_neighbour.shape[0]
    receivers = receiver_slot.shape[0]
    group_size = lax.axis_size("dom")
    rows = basis * quantities
    locals_ = stiffness.shape[0] + faces
    params = pltpu.CompilerParams(vmem_limit_bytes=60000 * 1024)

    element_row = jnp.arange(width, dtype=jnp.int32)[:, None]
    sent_live = jnp.arange(capacity)[None, :] < send_count[0][:, None]
    sent = jnp.where(sent_live, send_element[0], -1).reshape(-1)
    asked = jnp.concatenate([sent, receiver_element, jnp.full((LANES - receivers,), -1, jnp.int32)])
    select = (element_row == asked[None, :]).astype(BF16)
    choose_own = (element_row[None] == face_neighbour[:, None, :]).astype(BF16)
    halo_row = jnp.arange(slots * capacity, dtype=jnp.int32)[:, None] + width
    choose_halo = (halo_row[None] == face_neighbour[:, None, :]).astype(BF16)
    weights = jnp.pad(receiver_weight, ((0, 0), (0, LANES - receivers)))
    own_matrix = padded_k(jnp.concatenate([stiffness, -flux_local, -flux_remote], 0).reshape(-1, basis))
    halo_matrix = padded_k((-flux_remote).reshape(-1, basis))

    message = jax.ShapeDtypeStruct((SEND_ROWS, LANES), F32)
    values_shape = jax.ShapeDtypeStruct((quantities, LANES), F32)
    field_shape = jax.ShapeDtypeStruct((rows, width), F32)
    power_shape = jax.ShapeDtypeStruct((8, LANES), F32)
    outs = pl.pallas_call(
        first_kernel,
        out_shape=(field_shape,) + (message,) * slots + (values_shape,),
        in_specs=vmem(3),
        out_specs=tuple(vmem(slots + 2)),
        compiler_params=params,
        name="first_messages",
    )(element_state, select, weights)
    fields, messages = outs[0], outs[1:-1]

    powers = []
    samples = []
    for step in range(TIME_STEPS):
        last = step == TIME_STEPS - 1
        arrived = []
        for slot in range(slots):
            if slot < 2 * PEER_REACH:
                offset = slot + 1 if slot < PEER_REACH else PEER_REACH - 1 - slot
                pairs = [(i, (i + offset) % group_size) for i in range(group_size)]
                arrived.append(lax.ppermute(messages[slot], "dom", pairs))
            else:
                offset = 1 if slot == 2 * PEER_REACH else -1
                count = lax.axis_size("grp")
                pairs = [(i, i + offset) for i in range(count) if 0 <= i + offset < count]
                arrived.append(lax.ppermute(messages[slot], "grp", pairs))
        partial = pl.pallas_call(
            own_kernel,
            out_shape=field_shape,
            in_specs=vmem(6),
            out_specs=vmem(1)[0],
            scratch_shapes=[
                pltpu.VMEM((locals_ + faces, rows, width), F32),
                pltpu.VMEM((3 * HALF, width), BF16),
            ],
            compiler_params=params,
            cost_estimate=pl.CostEstimate(flops=8_000_000_000, bytes_accessed=10_000_000, transcendentals=0),
            name="own_terms",
        )(fields, own_matrix, star_matrix, face_local, face_remote, choose_own)
        field_out = jax.ShapeDtypeStruct(element_state.shape, F32) if last else field_shape
        sent_out = () if last else (message,) * slots
        chosen = select[:, slots * capacity :] if last else select
        outs = pl.pallas_call(
            lambda *refs, last=last: halo_kernel(last, *refs),
            out_shape=(field_out, power_shape, values_shape) + sent_out,
            in_specs=[pl.BlockSpec(memory_space=pltpu.SMEM)] + vmem(8 + slots),
            out_specs=tuple(vmem(3 + len(sent_out))),
            scratch_shapes=[
                pltpu.VMEM((rows, slots * capacity), F32),
                pltpu.VMEM((faces, rows, slots * capacity), F32),
                pltpu.VMEM((faces, rows, width), F32),
                pltpu.VMEM((3 * HALF, slots * capacity), BF16),
                pltpu.VMEM((rows, width), F32),
            ],
            compiler_params=params,
            cost_estimate=pl.CostEstimate(flops=6_000_000_000, bytes_accessed=10_000_000, transcendentals=0),
            name="halo_terms_last" if last else "halo_terms",
        )(element_count, fields, partial, halo_matrix, face_remote, choose_halo, energy_weight, chosen, weights, *arrived)
        fields, messages = outs[0], outs[3:]
        powers.append(outs[1])
        samples.append(outs[2])

    denominator = float(group_size * width * basis * quantities)
    own_energy = 0.5 * jnp.sum(jnp.stack(powers), axis=(1, 2))
    values = jnp.stack(samples)[:, :, :receivers].reshape(TIME_STEPS * quantities, receivers)
    matches = (receiver_slot[:, None] == jnp.arange(group_size * receivers)[None, :]).astype(F32)
    placed = jnp.dot(values, matches, precision=highest, preferred_element_type=F32)
    pieces = placed.reshape(-1, group_size, receivers).transpose(1, 0, 2).reshape(group_size, -1)
    fill = jnp.zeros((group_size, 16 - TIME_STEPS), F32)
    spread = jnp.broadcast_to(own_energy[None, :], (group_size, TIME_STEPS))
    pieces = jnp.concatenate([pieces, spread, fill], 1)
    arrived = lax.all_to_all(pieces, "dom", split_axis=0, concat_axis=0, tiled=True)
    total = arrived.sum(axis=0)
    traces = total[: TIME_STEPS * quantities * receivers].reshape(TIME_STEPS, quantities, receivers)
    energy = total[TIME_STEPS * quantities * receivers :][:TIME_STEPS] / denominator
    return (fields, energy[None, :], traces)


def solution(mesh):
    return jax.shard_map(
        per_device,
        mesh=mesh,
        in_specs=(
            P(None, None, GRP_DOM),
            P(),
            P(),
            P(),
            P(None, None, None, GRP_DOM),
            P(None, None, None, GRP_DOM),
            P(None, None, None, GRP_DOM),
            P(None, GRP_DOM),
            P(None, GRP_DOM),
            P(GRP_DOM),
            P(GRP_DOM, None),
            P(GRP_DOM, None, None),
            P(GRP_DOM),
            P(GRP_DOM),
            P(None, GRP_DOM),
        ),
        out_specs=(P(None, None, GRP_DOM), P("grp", None), P(None, None, GRP_DOM)),
        check_vma=False,
    )
```

```python
import jax
import jax.numpy as jnp
from jax import lax
from jax.experimental import pallas as pl
from jax.experimental.pallas import tpu as pltpu
from jax.sharding import PartitionSpec as P


PEER_REACH = 3
TIME_STEPS = 3
GRP_DOM = ("grp", "dom")
LANES = 128
HALF = 64
SEND_ROWS = 256
FIRST_SENDS = (6, 7, 0, 1, 5)
F32 = jnp.float32
BF16 = jnp.bfloat16
highest = lax.Precision.HIGHEST


def two_parts(value):
    high = value.astype(BF16)
    low = (value - high.astype(F32)).astype(BF16)
    return high, low


def dot(a, b):
    return jnp.dot(a, b, preferred_element_type=F32)


def padded_k(matrices):
    rounded = lax.reduce_precision(matrices, 8, 7)
    low = matrices - rounded
    total = jnp.zeros((matrices.shape[0], 3 * HALF), F32)
    for part, value in enumerate((rounded, rounded, low)):
        after = 3 * HALF - part * HALF - matrices.shape[1]
        total = total + jnp.pad(value, ((0, 0), (part * HALF, after)))
    return total.astype(BF16)


def stack_columns(field, rhs_ref):
    basis = field.shape[0]
    high, low = two_parts(field)
    rhs_ref[0:basis, :] = high
    rhs_ref[HALF : HALF + basis, :] = low
    rhs_ref[2 * HALF : 2 * HALF + basis, :] = high


def clear_fill(rhs_ref, basis):
    for part in range(3):
        rhs_ref[part * HALF + basis : (part + 1) * HALF, :] = jnp.zeros(
            (HALF - basis, rhs_ref.shape[1]), BF16
        )


def pick(field, chosen):
    high, low = two_parts(field)
    return dot(high, chosen) + dot(low, chosen)


def apply_maps(tile, matrices, base, emit, quantities, basis):
    lanes = pl.ds(pl.multiple_of(tile * LANES, LANES), LANES)
    group = 3
    for first in range(0, quantities, group):

        def column(q, total):
            total = list(total)
            rows = pl.ds(pl.multiple_of(q * basis, 8), basis)
            for ref, at, sign, terms_ref, slot in matrices:
                term = terms_ref[slot, rows, lanes]
                for k in range(group):
                    product = ref[first + k, q, at : at + 1, lanes] * term
                    total[k] = total[k] + product if sign > 0 else total[k] - product
            return tuple(total)

        start = tuple(base(first + k, lanes) for k in range(group))
        total = lax.fori_loop(0, quantities, column, start)
        for k in range(group):
            emit(first + k, lanes, total[k])


def pack(field, select_ref, weight_ref, message_refs, values_ref, quantities, basis):
    rows = quantities * basis
    lane = lax.broadcasted_iota(jnp.int32, (SEND_ROWS, LANES), 1) < HALF
    tail = SEND_ROWS - (rows - SEND_ROWS)
    pairs = len(message_refs) // 2
    receivers = weight_ref.shape[1]
    if not pairs:
        picked = pick(field, select_ref[:, select_ref.shape[1] - LANES :])
    else:
        picked = pick(field, select_ref[...])
    for pair in range(pairs):
        block = picked[:, pair * LANES : (pair + 1) * LANES]
        top = block[:SEND_ROWS]
        bottom = jnp.concatenate([block[SEND_ROWS:], jnp.zeros((tail, LANES), F32)], 0)
        message_refs[2 * pair][...] = jnp.where(lane, top, pltpu.roll(bottom, HALF, 1))
        message_refs[2 * pair + 1][...] = jnp.where(lane, pltpu.roll(top, HALF, 1), bottom)
    block = picked[:, pairs * LANES : pairs * LANES + receivers]
    for q in range(quantities):
        values_ref[q : q + 1, :] = jnp.sum(
            block[q * basis : (q + 1) * basis] * weight_ref[...], axis=0, keepdims=True
        )


def first_kernel(count_ref, field_ref, send_ref, receiver_ref, weight_ref, select_ref, *messages):
    rows, width = field_ref.shape
    basis = weight_ref.shape[0]
    slots, capacity = send_ref.shape
    receivers = receiver_ref.shape[1]
    select_ref[:, slots * capacity :] = jnp.zeros((width, LANES), BF16)
    element = lax.broadcasted_iota(jnp.int32, (width, capacity), 0)
    place = lax.broadcasted_iota(jnp.int32, (1, capacity), 1)
    for slot in range(slots):
        asked = jnp.where(place < count_ref[0, slot], send_ref[slot : slot + 1, :], -1)
        select_ref[:, slot * capacity : (slot + 1) * capacity] = jnp.where(
            element == asked, 1.0, 0.0
        ).astype(BF16)
    element = lax.broadcasted_iota(jnp.int32, (width, receivers), 0)
    select_ref[:, slots * capacity : slots * capacity + receivers] = jnp.where(
        element == receiver_ref[...], 1.0, 0.0
    ).astype(BF16)
    values_ref = messages[-1]
    pack(field_ref[...], select_ref, weight_ref, messages[:-1], values_ref, rows // basis, basis)


def own_kernel_a(field_ref, matrix_ref, choose_ref, terms_ref, gathered_ref, rhs_ref):
    faces = choose_ref.shape[0]
    locals_, rows_all, width = terms_ref.shape
    basis = matrix_ref.shape[0] // (locals_ + faces)
    quantities = rows_all // basis
    clear_fill(rhs_ref, basis)

    def modal(q, carry):
        rows = pl.ds(pl.multiple_of(q * basis, 8), basis)
        stack_columns(field_ref[rows, :], rhs_ref)
        for at in range(0, width, 2 * LANES):
            lanes = slice(at, min(at + 2 * LANES, width))
            result = dot(matrix_ref[...], rhs_ref[:, lanes])
            for n in range(locals_):
                terms_ref[n, rows, lanes] = result[n * basis : (n + 1) * basis]
            for f in range(faces):
                n = locals_ + f
                gathered_ref[f, rows, lanes] = result[n * basis : (n + 1) * basis]
        return carry

    lax.fori_loop(0, quantities, modal, 0)

    def gather(f, carry):
        gathered_ref[f] = pick(gathered_ref[f], choose_ref[f])
        return carry

    lax.fori_loop(0, faces, gather, 0)


def own_kernel_b(field_ref, terms_ref, star_ref, local_ref, out_ref):
    quantities, _, stars, width = star_ref.shape
    basis = field_ref.shape[0] // quantities
    matrices = [(star_ref, n, 1, terms_ref, n) for n in range(stars)] + [
        (local_ref, f, -1, terms_ref, stars + f) for f in range(local_ref.shape[2])
    ]

    def tile_body(tile, carry):
        def base(p, lanes):
            return field_ref[p * basis : (p + 1) * basis, lanes]

        def emit(p, lanes, value):
            out_ref[p * basis : (p + 1) * basis, lanes] = value

        apply_maps(tile, matrices, base, emit, quantities, basis)
        return carry

    lax.fori_loop(0, width // LANES, tile_body, 0)


def halo_kernel(slots, sends, live_ref, field_ref, partial_ref, gathered_ref, matrix_ref, remote_ref, choose_ref, energy_ref, select_ref, weight_ref, *rest):
    halo_refs = rest[:slots]
    state_ref, power_ref, values_ref = rest[slots : slots + 3]
    messages = rest[slots + 3 : slots + 3 + sends]
    columns_ref, flux_ref, terms_ref, rhs_ref = rest[slots + 3 + sends :]
    quantities, _, faces = remote_ref.shape[:3]
    rows_all, width = field_ref.shape
    basis = rows_all // quantities
    clear_fill(rhs_ref, basis)
    lane = lax.broadcasted_iota(jnp.int32, (SEND_ROWS, LANES), 1) < HALF
    for pair in range(slots // 2):
        a = halo_refs[2 * pair][...]
        b = halo_refs[2 * pair + 1][...]
        lanes = slice(pair * LANES, (pair + 1) * LANES)
        columns_ref[0:SEND_ROWS, lanes] = jnp.where(lane, a, pltpu.roll(b, HALF, 1))
        bottom = jnp.where(lane, pltpu.roll(a, HALF, 1), b)
        columns_ref[SEND_ROWS:, lanes] = bottom[: rows_all - SEND_ROWS]

    def modal(q, carry):
        rows = pl.ds(pl.multiple_of(q * basis, 8), basis)
        stack_columns(columns_ref[rows, :], rhs_ref)
        result = dot(matrix_ref[...], rhs_ref[...])
        for f in range(faces):
            flux_ref[f, rows, :] = result[f * basis : (f + 1) * basis]
        return carry

    lax.fori_loop(0, quantities, modal, 0)

    def gather(f, carry):
        terms_ref[f] = gathered_ref[f] + pick(flux_ref[f], choose_ref[f])
        return carry

    lax.fori_loop(0, faces, gather, 0)
    matrices = [(remote_ref, f, -1, terms_ref, f) for f in range(faces)]

    def tile_body(tile, power):
        totals = [power]

        def base(p, lanes):
            return partial_ref[p * basis : (p + 1) * basis, lanes]

        def emit(p, lanes, value):
            live = live_ref[0:1, lanes] > 0
            kept = jnp.where(live, value, field_ref[p * basis : (p + 1) * basis, lanes])
            state_ref[p * basis : (p + 1) * basis, lanes] = kept
            squares = kept * kept * energy_ref[p : p + 1, lanes]
            for block in range(basis // 8):
                totals[0] = totals[0] + squares[block * 8 : (block + 1) * 8]

        apply_maps(tile, matrices, base, emit, quantities, basis)
        return totals[0]

    power_ref[...] = lax.fori_loop(0, width // LANES, tile_body, jnp.zeros((8, LANES), F32))
    pack(state_ref[...], select_ref, weight_ref, messages, values_ref, quantities, basis)


def vmem(count):
    return [pl.BlockSpec(memory_space=pltpu.VMEM)] * count


def smem(count):
    return [pl.BlockSpec(memory_space=pltpu.SMEM)] * count


def granted(mib, flops=0):
    extra = {}
    if flops:
        extra["cost_estimate"] = pl.CostEstimate(flops=flops, bytes_accessed=8_000_000, transcendentals=0)
    return dict(compiler_params=pltpu.CompilerParams(vmem_limit_bytes=mib * 2**20), **extra)


def per_device(
    element_state,
    stiffness,
    flux_local,
    flux_remote,
    star_matrix,
    face_local,
    face_remote,
    energy_weight,
    face_neighbour,
    element_count,
    send_count,
    send_element,
    receiver_element,
    receiver_slot,
    receiver_weight,
):
    basis, quantities, width = element_state.shape
    slots, capacity = send_element.shape[1:]
    faces = face_neighbour.shape[0]
    receivers = receiver_slot.shape[0]
    group_size = lax.axis_size("dom")
    rows = basis * quantities
    locals_ = stiffness.shape[0] + faces
    halo_width = slots * capacity

    fields = element_state.transpose(1, 0, 2).reshape(rows, width)
    star = star_matrix.transpose(1, 2, 0, 3)
    local = face_local.transpose(1, 2, 0, 3)
    remote = face_remote.transpose(1, 2, 0, 3)

    message = jax.ShapeDtypeStruct((SEND_ROWS, LANES), F32)
    values_shape = jax.ShapeDtypeStruct((quantities, receivers), F32)
    field_shape = jax.ShapeDtypeStruct((rows, width), F32)
    power_shape = jax.ShapeDtypeStruct((8, LANES), F32)
    terms_shape = jax.ShapeDtypeStruct((locals_, rows, width), F32)
    gathered_shape = jax.ShapeDtypeStruct((faces, rows, width), F32)
    select_shape = jax.ShapeDtypeStruct((width, halo_width + LANES), BF16)
    outs = pl.pallas_call(
        first_kernel,
        out_shape=(select_shape,) + (message,) * slots + (values_shape,),
        in_specs=smem(1) + vmem(4),
        out_specs=tuple(vmem(slots + 2)),
        name="first_messages",
        **granted(16),
    )(send_count, fields, send_element[0], receiver_element[None, :], receiver_weight)
    select, messages = outs[0], outs[1:-1]

    element_row = jnp.arange(width, dtype=jnp.int32)[:, None]
    choose_own = (element_row[None] == face_neighbour[:, None, :]).astype(BF16)
    halo_row = jnp.arange(halo_width, dtype=jnp.int32)[:, None] + width
    choose_halo = (halo_row[None] == face_neighbour[:, None, :]).astype(BF16)
    own_matrix = padded_k(jnp.concatenate([stiffness, flux_local, flux_remote], 0).reshape(-1, basis))
    halo_matrix = own_matrix[locals_ * basis :]

    live = (jnp.arange(width, dtype=jnp.int32) < element_count[0]).astype(F32)[None, :]
    live_energy = jnp.where(live > 0, energy_weight, 0.0)

    def send(slot, value):
        if slot < 2 * PEER_REACH:
            offset = slot + 1 if slot < PEER_REACH else PEER_REACH - 1 - slot
            pairs = [(i, (i + offset) % group_size) for i in range(group_size)]
            return lax.ppermute(value, "dom", pairs)
        offset = 1 if slot == 2 * PEER_REACH else -1
        count = lax.axis_size("grp")
        pairs = [(i, i + offset) for i in range(count) if 0 <= i + offset < count]
        return lax.ppermute(value, "grp", pairs)

    powers = []
    samples = []
    for step in range(TIME_STEPS):
        last = step == TIME_STEPS - 1
        arrived = [None] * slots
        for slot in FIRST_SENDS:
            arrived[slot] = send(slot, messages[slot])
        terms, gathered = pl.pallas_call(
            own_kernel_a,
            out_shape=(terms_shape, gathered_shape),
            in_specs=vmem(3),
            out_specs=tuple(vmem(2)),
            scratch_shapes=[pltpu.VMEM((3 * HALF, width), BF16)],
            name="own_terms_a",
            **granted(8, 5_000_000_000),
        )(fields, own_matrix, choose_own)
        others = [slot for slot in range(slots) if slot not in FIRST_SENDS]
        held = lax.optimization_barrier(tuple(messages[slot] for slot in others) + (gathered,))
        gathered = held[-1]
        for slot, value in zip(others, held):
            arrived[slot] = send(slot, value)
        partial = pl.pallas_call(
            own_kernel_b,
            out_shape=field_shape,
            in_specs=vmem(4),
            out_specs=vmem(1)[0],
            name="own_terms_b",
            **granted(4, 5_000_000_000),
        )(fields, terms, star, local)
        sends = 0 if last else slots
        outs = pl.pallas_call(
            lambda *refs, sends=sends: halo_kernel(slots, sends, *refs),
            out_shape=(field_shape, power_shape, values_shape) + (message,) * sends,
            in_specs=vmem(10 + slots),
            out_specs=tuple(vmem(3 + sends)),
            scratch_shapes=[
                pltpu.VMEM((rows, halo_width), F32),
                pltpu.VMEM((faces, rows, halo_width), F32),
                pltpu.VMEM((faces, rows, width), F32),
                pltpu.VMEM((3 * HALF, halo_width), BF16),
            ],
            name="halo_terms_last" if last else "halo_terms",
            **granted(18, 6_000_000_000),
        )(live, fields, partial, gathered, halo_matrix, remote, choose_halo, live_energy, select, receiver_weight, *arrived)
        fields, messages = outs[0], outs[3:]
        powers.append(outs[1])
        samples.append(outs[2])

    new_state = fields.reshape(quantities, basis, width).transpose(1, 0, 2)
    denominator = float(group_size * width * basis * quantities)
    own_energy = 0.5 * jnp.sum(jnp.stack(powers), axis=(1, 2))
    values = jnp.concatenate(samples, 0)
    matches = (receiver_slot[:, None] == jnp.arange(group_size * receivers)[None, :]).astype(F32)
    placed = jnp.dot(values, matches, precision=highest, preferred_element_type=F32)
    pieces = placed.reshape(-1, group_size, receivers).transpose(1, 0, 2).reshape(group_size, -1)
    fill = jnp.zeros((group_size, 16 - TIME_STEPS), F32)
    spread = jnp.broadcast_to(own_energy[None, :], (group_size, TIME_STEPS))
    pieces = jnp.concatenate([pieces, spread, fill], 1)
    arrived = lax.all_to_all(pieces, "dom", split_axis=0, concat_axis=0, tiled=True)
    total = arrived.sum(axis=0)
    traces = total[: TIME_STEPS * quantities * receivers].reshape(TIME_STEPS, quantities, receivers)
    energy = total[TIME_STEPS * quantities * receivers :][:TIME_STEPS] / denominator
    return (new_state, energy[None, :], traces)


def solution(mesh):
    return jax.shard_map(
        per_device,
        mesh=mesh,
        in_specs=(
            P(None, None, GRP_DOM),
            P(),
            P(),
            P(),
            P(None, None, None, GRP_DOM),
            P(None, None, None, GRP_DOM),
            P(None, None, None, GRP_DOM),
            P(None, GRP_DOM),
            P(None, GRP_DOM),
            P(GRP_DOM),
            P(GRP_DOM, None),
            P(GRP_DOM, None, None),
            P(GRP_DOM),
            P(GRP_DOM),
            P(None, GRP_DOM),
        ),
        out_specs=(P(None, None, GRP_DOM), P("grp", None), P(None, None, GRP_DOM)),
        check_vma=False,
    )
```

```python
import jax
import jax.numpy as jnp
from jax import lax
from jax.experimental import pallas as pl
from jax.experimental.pallas import tpu as pltpu
from jax.sharding import PartitionSpec as P


PEER_REACH = 3
TIME_STEPS = 3
GRP_DOM = ("grp", "dom")
LANES = 128
HALF = 64
SEND_ROWS = 256
FIRST_SENDS = (6, 7, 0, 1, 5)
F32 = jnp.float32
BF16 = jnp.bfloat16
highest = lax.Precision.HIGHEST


def two_parts(value):
    high = value.astype(BF16)
    low = (value - high.astype(F32)).astype(BF16)
    return high, low


def dot(a, b):
    return jnp.dot(a, b, preferred_element_type=F32)


def padded_k(matrices):
    rounded = lax.reduce_precision(matrices, 8, 7)
    low = matrices - rounded
    total = jnp.zeros((matrices.shape[0], 3 * HALF), F32)
    for part, value in enumerate((rounded, rounded, low)):
        after = 3 * HALF - part * HALF - matrices.shape[1]
        total = total + jnp.pad(value, ((0, 0), (part * HALF, after)))
    return total.astype(BF16)


def stack_columns(field, rhs_ref):
    basis = field.shape[0]
    high, low = two_parts(field)
    rhs_ref[0:basis, :] = high
    rhs_ref[HALF : HALF + basis, :] = low
    rhs_ref[2 * HALF : 2 * HALF + basis, :] = high


def clear_fill(rhs_ref, basis):
    for part in range(3):
        rhs_ref[part * HALF + basis : (part + 1) * HALF, :] = jnp.zeros(
            (HALF - basis, rhs_ref.shape[1]), BF16
        )


def pick_parts(high, low, chosen):
    width = high.shape[1]
    body = width - LANES
    ends = jnp.concatenate([high[:, body:], low[:, body:]], 1)
    return dot(high[:, :body], chosen[:body]) + dot(low[:, :body], chosen[:body]) + dot(ends, chosen[body:])


def pick(field, chosen):
    high, low = two_parts(field)
    if chosen.shape[0] > field.shape[1]:
        return pick_parts(high, low, chosen)
    return dot(high, chosen) + dot(low, chosen)


def apply_maps(unit, matrices, base, emit, quantities, basis, unroll):
    group = 3
    tile, part = unit // group, unit % group
    lanes = pl.ds(pl.multiple_of(tile * LANES, LANES), LANES)

    def column(q, total):
        total = list(total)
        rows = pl.ds(pl.multiple_of(q * basis, 8), basis)
        for ref, at, sign, terms_ref, slot in matrices:
            term = terms_ref[slot, rows, lanes]
            for k in range(group):
                product = ref[group * part + k, q, at : at + 1, lanes] * term
                total[k] = total[k] + product if sign > 0 else total[k] - product
        return tuple(total)

    def rows_of(k):
        return pl.ds(pl.multiple_of((group * part + k) * basis, 8), basis)

    total = tuple(base(rows_of(k), lanes) for k in range(group))
    if unroll:
        for q in range(quantities):
            total = column(q, total)
    else:
        total = lax.fori_loop(0, quantities, column, total)
    for k in range(group):
        emit(rows_of(k), lanes, total[k])


def apply_tile(tile, matrices, base, emit, quantities, basis):
    lanes = pl.ds(pl.multiple_of(tile * LANES, LANES), LANES)
    group = 3
    for first in range(0, quantities, group):

        def column(q, total):
            total = list(total)
            rows = pl.ds(pl.multiple_of(q * basis, 8), basis)
            for ref, at, sign, terms_ref, slot in matrices:
                term = terms_ref[slot, rows, lanes]
                for k in range(group):
                    product = ref[first + k, q, at : at + 1, lanes] * term
                    total[k] = total[k] + product if sign > 0 else total[k] - product
            return tuple(total)

        start = tuple(base(first + k, lanes) for k in range(group))
        total = lax.fori_loop(0, quantities, column, start)
        for k in range(group):
            emit(first + k, lanes, total[k])


def pack(field, select_ref, weight_ref, message_refs, values_ref, quantities, basis):
    rows = quantities * basis
    lane = lax.broadcasted_iota(jnp.int32, (SEND_ROWS, LANES), 1) < HALF
    tail = SEND_ROWS - (rows - SEND_ROWS)
    pairs = len(message_refs) // 2
    receivers = weight_ref.shape[1]
    if not pairs:
        picked = pick(field, select_ref[:, select_ref.shape[1] - LANES :])
    else:
        picked = pick(field, select_ref[...])
    for pair in range(pairs):
        block = picked[:, pair * LANES : (pair + 1) * LANES]
        top = block[:SEND_ROWS]
        bottom = jnp.concatenate([block[SEND_ROWS:], jnp.zeros((tail, LANES), F32)], 0)
        message_refs[2 * pair][...] = jnp.where(lane, top, pltpu.roll(bottom, HALF, 1))
        message_refs[2 * pair + 1][...] = jnp.where(lane, pltpu.roll(top, HALF, 1), bottom)
    block = picked[:, pairs * LANES : pairs * LANES + receivers]
    for q in range(quantities):
        values_ref[q : q + 1, :] = jnp.sum(
            block[q * basis : (q + 1) * basis] * weight_ref[...], axis=0, keepdims=True
        )


def first_kernel(count_ref, field_ref, send_ref, receiver_ref, weight_ref, select_ref, *messages):
    rows = field_ref.shape[0]
    width = select_ref.shape[0]
    basis = weight_ref.shape[0]
    slots, capacity = send_ref.shape
    receivers = receiver_ref.shape[1]
    select_ref[:, slots * capacity :] = jnp.zeros((width, LANES), BF16)
    element = lax.broadcasted_iota(jnp.int32, (width, capacity), 0)
    element = jnp.where(element < field_ref.shape[1], element, element - LANES)
    place = lax.broadcasted_iota(jnp.int32, (1, capacity), 1)
    for slot in range(slots):
        asked = jnp.where(place < count_ref[0, slot], send_ref[slot : slot + 1, :], -1)
        select_ref[:, slot * capacity : (slot + 1) * capacity] = jnp.where(
            element == asked, 1.0, 0.0
        ).astype(BF16)
    element = lax.broadcasted_iota(jnp.int32, (width, receivers), 0)
    element = jnp.where(element < field_ref.shape[1], element, element - LANES)
    select_ref[:, slots * capacity : slots * capacity + receivers] = jnp.where(
        element == receiver_ref[...], 1.0, 0.0
    ).astype(BF16)
    values_ref = messages[-1]
    pack(field_ref[...], select_ref, weight_ref, messages[:-1], values_ref, rows // basis, basis)


def own_maps(star_ref, local_ref, terms_ref):
    stars = star_ref.shape[2]
    return [(star_ref, n, 1, terms_ref, n) for n in range(stars)] + [
        (local_ref, f, -1, terms_ref, stars + f) for f in range(local_ref.shape[2])
    ]


def own_kernel_a(field_ref, matrix_ref, star_ref, local_ref, terms_ref, high_ref, low_ref, out_ref, rhs_ref, flux_ref):
    faces = high_ref.shape[0]
    locals_, rows_all, width = terms_ref.shape
    basis = matrix_ref.shape[0] // (locals_ + faces)
    quantities = rows_all // basis
    clear_fill(rhs_ref, basis)

    def modal(first, count):
        for k in range(count):
            rows = pl.ds(pl.multiple_of((first + k) * basis, 8), basis)
            stack_columns(field_ref[rows, :], rhs_ref.at[:, k * width : (k + 1) * width])
        for at in range(0, count * width, 2 * LANES):
            end = min(at + 2 * LANES, count * width)
            result = dot(matrix_ref[...], rhs_ref[:, at:end])
            for low in range(at, end, LANES):
                k, lane = low // width, low % width
                rows = pl.ds(pl.multiple_of((first + k) * basis, 8), basis)
                for n in range(locals_ + faces):
                    value = result[n * basis : (n + 1) * basis, low - at : low - at + LANES]
                    if n < locals_:
                        terms_ref[n, rows, lane : lane + LANES] = value
                    else:
                        flux_ref[n - locals_, rows, lane : lane + LANES] = value

    def pair(i, carry):
        modal(2 * i, 2)
        return carry

    lax.fori_loop(0, quantities // 2, pair, 0)
    if quantities % 2:
        modal(quantities - 1, 1)

    def parts(f, carry):
        high_ref[f], low_ref[f] = two_parts(flux_ref[f])
        return carry

    lax.fori_loop(0, faces, parts, 0)

    def base(rows, lanes):
        return field_ref[rows, lanes]

    def emit(rows, lanes, value):
        out_ref[rows, :] = value

    def plain(unit, carry):
        apply_maps(unit, own_maps(star_ref, local_ref, terms_ref), base, emit, quantities, basis, False)
        return carry

    units = 3 * width // LANES
    lax.fori_loop(units - 3, units, plain, 0)


def own_kernel_b(field_ref, terms_ref, star_ref, local_ref, high_ref, low_ref, choose_ref, out_ref, gathered_ref):
    quantities = star_ref.shape[0]
    basis = field_ref.shape[0] // quantities

    def base(rows, lanes):
        return field_ref[rows, lanes]

    def emit(rows, lanes, value):
        out_ref[rows, lanes] = value

    def face(f, carry):
        gathered_ref[f] = pick_parts(high_ref[f], low_ref[f], choose_ref[f])
        for k in range(3):
            apply_maps(3 * f + k, own_maps(star_ref, local_ref, terms_ref), base, emit, quantities, basis, True)
        return carry

    lax.fori_loop(0, high_ref.shape[0], face, 0)


def halo_kernel(slots, sends, live_ref, field_ref, partial_ref, partial_b_ref, gathered_ref, matrix_ref, remote_ref, choose_ref, energy_ref, select_ref, weight_ref, *rest):
    halo_refs = rest[:slots]
    state_ref, power_ref, values_ref = rest[slots : slots + 3]
    messages = rest[slots + 3 : slots + 3 + sends]
    columns_ref, flux_ref, terms_ref, rhs_ref = rest[slots + 3 + sends :]
    quantities, _, faces = remote_ref.shape[:3]
    rows_all, width = field_ref.shape
    basis = rows_all // quantities
    clear_fill(rhs_ref, basis)
    lane = lax.broadcasted_iota(jnp.int32, (SEND_ROWS, LANES), 1) < HALF
    for pair in range(slots // 2):
        a = halo_refs[2 * pair][...]
        b = halo_refs[2 * pair + 1][...]
        lanes = slice(pair * LANES, (pair + 1) * LANES)
        columns_ref[0:SEND_ROWS, lanes] = jnp.where(lane, a, pltpu.roll(b, HALF, 1))
        bottom = jnp.where(lane, pltpu.roll(a, HALF, 1), b)
        columns_ref[SEND_ROWS:, lanes] = bottom[: rows_all - SEND_ROWS]

    def modal(q, carry):
        rows = pl.ds(pl.multiple_of(q * basis, 8), basis)
        stack_columns(columns_ref[rows, :], rhs_ref)
        result = dot(matrix_ref[...], rhs_ref[...])
        for f in range(faces):
            flux_ref[f, rows, :] = result[f * basis : (f + 1) * basis]
        return carry

    lax.fori_loop(0, quantities, modal, 0)

    def gather(f, carry):
        terms_ref[f] = gathered_ref[f] + pick(flux_ref[f], choose_ref[f])
        return carry

    lax.fori_loop(0, faces, gather, 0)
    matrices = [(remote_ref, f, -1, terms_ref, f) for f in range(faces)]

    def tile_body(partial_ref, first, tile, power):
        totals = [power]
        own = pl.ds(pl.multiple_of((tile - first) * LANES, LANES), LANES)

        def base(p, lanes):
            return partial_ref[p * basis : (p + 1) * basis, own]

        def emit(p, lanes, value):
            live = live_ref[0:1, lanes] > 0
            kept = jnp.where(live, value, field_ref[p * basis : (p + 1) * basis, lanes])
            state_ref[p * basis : (p + 1) * basis, lanes] = kept
            squares = kept * kept * energy_ref[p : p + 1, lanes]
            for block in range(basis // 8):
                totals[0] = totals[0] + squares[block * 8 : (block + 1) * 8]

        apply_tile(tile, matrices, base, emit, quantities, basis)
        return totals[0]

    tiles = width // LANES
    power = jnp.zeros((8, LANES), F32)
    power = lax.fori_loop(0, tiles - 1, lambda tile, power: tile_body(partial_ref, 0, tile, power), power)
    power_ref[...] = tile_body(partial_b_ref, tiles - 1, tiles - 1, power)
    pack(state_ref[...], select_ref, weight_ref, messages, values_ref, quantities, basis)


def vmem(count):
    return [pl.BlockSpec(memory_space=pltpu.VMEM)] * count


def smem(count):
    return [pl.BlockSpec(memory_space=pltpu.SMEM)] * count


def granted(mib, flops=0):
    extra = {}
    if flops:
        extra["cost_estimate"] = pl.CostEstimate(flops=flops, bytes_accessed=8_000_000, transcendentals=0)
    return dict(compiler_params=pltpu.CompilerParams(vmem_limit_bytes=mib * 2**20), **extra)


def per_device(
    element_state,
    stiffness,
    flux_local,
    flux_remote,
    star_matrix,
    face_local,
    face_remote,
    energy_weight,
    face_neighbour,
    element_count,
    send_count,
    send_element,
    receiver_element,
    receiver_slot,
    receiver_weight,
):
    basis, quantities, width = element_state.shape
    slots, capacity = send_element.shape[1:]
    faces = face_neighbour.shape[0]
    receivers = receiver_slot.shape[0]
    group_size = lax.axis_size("dom")
    rows = basis * quantities
    locals_ = stiffness.shape[0] + faces
    halo_width = slots * capacity

    fields = element_state.transpose(1, 0, 2).reshape(rows, width)
    star = star_matrix.transpose(1, 2, 0, 3)
    local = face_local.transpose(1, 2, 0, 3)
    remote = face_remote.transpose(1, 2, 0, 3)

    message = jax.ShapeDtypeStruct((SEND_ROWS, LANES), F32)
    values_shape = jax.ShapeDtypeStruct((quantities, receivers), F32)
    field_shape = jax.ShapeDtypeStruct((rows, width), F32)
    power_shape = jax.ShapeDtypeStruct((8, LANES), F32)
    terms_shape = jax.ShapeDtypeStruct((locals_, rows, width), F32)
    parts_shape = jax.ShapeDtypeStruct((faces, rows, width), BF16)
    gathered_shape = jax.ShapeDtypeStruct((faces, rows, width), F32)
    select_shape = jax.ShapeDtypeStruct((width + LANES, halo_width + LANES), BF16)
    outs = pl.pallas_call(
        first_kernel,
        out_shape=(select_shape,) + (message,) * slots + (values_shape,),
        in_specs=smem(1) + vmem(4),
        out_specs=tuple(vmem(slots + 2)),
        name="first_messages",
        **granted(16),
    )(send_count, fields, send_element[0], receiver_element[None, :], receiver_weight)
    select, messages = outs[0], outs[1:-1]

    element_row = jnp.arange(width + LANES, dtype=jnp.int32)[:, None]
    element_row = jnp.where(element_row < width, element_row, element_row - LANES)
    choose_own = (element_row[None] == face_neighbour[:, None, :]).astype(BF16)
    halo_row = jnp.arange(halo_width, dtype=jnp.int32)[:, None] + width
    choose_halo = (halo_row[None] == face_neighbour[:, None, :]).astype(BF16)
    own_matrix = padded_k(jnp.concatenate([stiffness, flux_local, flux_remote], 0).reshape(-1, basis))
    halo_matrix = own_matrix[locals_ * basis :]

    live = (jnp.arange(width, dtype=jnp.int32) < element_count[0]).astype(F32)[None, :]
    live_energy = jnp.where(live > 0, energy_weight, 0.0)

    def send(slot, value):
        if slot < 2 * PEER_REACH:
            offset = slot + 1 if slot < PEER_REACH else PEER_REACH - 1 - slot
            pairs = [(i, (i + offset) % group_size) for i in range(group_size)]
            return lax.ppermute(value, "dom", pairs)
        offset = 1 if slot == 2 * PEER_REACH else -1
        count = lax.axis_size("grp")
        pairs = [(i, i + offset) for i in range(count) if 0 <= i + offset < count]
        return lax.ppermute(value, "grp", pairs)

    powers = []
    samples = []
    for step in range(TIME_STEPS):
        last = step == TIME_STEPS - 1
        arrived = [None] * slots
        for slot in FIRST_SENDS:
            arrived[slot] = send(slot, messages[slot])
        terms, high, low, partial_b = pl.pallas_call(
            own_kernel_a,
            out_shape=(terms_shape, parts_shape, parts_shape, jax.ShapeDtypeStruct((rows, LANES), F32)),
            in_specs=vmem(4),
            out_specs=tuple(vmem(4)),
            scratch_shapes=[pltpu.VMEM((3 * HALF, 2 * width), BF16), pltpu.VMEM((faces, rows, width), F32)],
            name="own_terms_a",
            **granted(10, 5_000_000_000),
        )(fields, own_matrix, star, local)
        others = [slot for slot in range(slots) if slot not in FIRST_SENDS]
        held = lax.optimization_barrier(tuple(messages[slot] for slot in others) + (partial_b,))
        partial_b = held[-1]
        for slot, value in zip(others, held):
            arrived[slot] = send(slot, value)
        partial, gathered = pl.pallas_call(
            own_kernel_b,
            out_shape=(jax.ShapeDtypeStruct((rows, width - LANES), F32), gathered_shape),
            in_specs=vmem(7),
            out_specs=tuple(vmem(2)),
            name="own_terms_b",
            **granted(6, 5_000_000_000),
        )(fields, terms, star, local, high, low, choose_own)
        sends = 0 if last else slots
        outs = pl.pallas_call(
            lambda *refs, sends=sends: halo_kernel(slots, sends, *refs),
            out_shape=(field_shape, power_shape, values_shape) + (message,) * sends,
            in_specs=vmem(11 + slots),
            out_specs=tuple(vmem(3 + sends)),
            scratch_shapes=[
                pltpu.VMEM((rows, halo_width), F32),
                pltpu.VMEM((faces, rows, halo_width), F32),
                pltpu.VMEM((faces, rows, width), F32),
                pltpu.VMEM((3 * HALF, halo_width), BF16),
            ],
            name="halo_terms_last" if last else "halo_terms",
            **granted(18, 6_000_000_000),
        )(live, fields, partial, partial_b, gathered, halo_matrix, remote, choose_halo, live_energy, select, receiver_weight, *arrived)
        fields, messages = outs[0], outs[3:]
        powers.append(outs[1])
        samples.append(outs[2])

    new_state = fields.reshape(quantities, basis, width).transpose(1, 0, 2)
    denominator = float(group_size * width * basis * quantities)
    own_energy = 0.5 * jnp.sum(jnp.stack(powers), axis=(1, 2))
    values = jnp.concatenate(samples, 0)
    matches = (receiver_slot[:, None] == jnp.arange(group_size * receivers)[None, :]).astype(F32)
    placed = jnp.dot(values, matches, precision=highest, preferred_element_type=F32)
    pieces = placed.reshape(-1, group_size, receivers).transpose(1, 0, 2).reshape(group_size, -1)
    fill = jnp.zeros((group_size, 16 - TIME_STEPS), F32)
    spread = jnp.broadcast_to(own_energy[None, :], (group_size, TIME_STEPS))
    pieces = jnp.concatenate([pieces, spread, fill], 1)
    arrived = lax.all_to_all(pieces, "dom", split_axis=0, concat_axis=0, tiled=True)
    total = arrived.sum(axis=0)
    traces = total[: TIME_STEPS * quantities * receivers].reshape(TIME_STEPS, quantities, receivers)
    energy = total[TIME_STEPS * quantities * receivers :][:TIME_STEPS] / denominator
    return (new_state, energy[None, :], traces)


def solution(mesh):
    return jax.shard_map(
        per_device,
        mesh=mesh,
        in_specs=(
            P(None, None, GRP_DOM),
            P(),
            P(),
            P(),
            P(None, None, None, GRP_DOM),
            P(None, None, None, GRP_DOM),
            P(None, None, None, GRP_DOM),
            P(None, GRP_DOM),
            P(None, GRP_DOM),
            P(GRP_DOM),
            P(GRP_DOM, None),
            P(GRP_DOM, None, None),
            P(GRP_DOM),
            P(GRP_DOM),
            P(None, GRP_DOM),
        ),
        out_specs=(P(None, None, GRP_DOM), P("grp", None), P(None, None, GRP_DOM)),
        check_vma=False,
    )
```

```python
import jax
import jax.numpy as jnp
from jax import lax
from jax.experimental import pallas as pl
from jax.experimental.pallas import tpu as pltpu
from jax.sharding import PartitionSpec as P


PEER_REACH = 3
TIME_STEPS = 3
GRP_DOM = ("grp", "dom")
LANES = 128
HALF = 64
SEND_ROWS = 256
FIRST_SENDS = (6, 7, 0, 1, 5)
F32 = jnp.float32
BF16 = jnp.bfloat16
highest = lax.Precision.HIGHEST


def two_parts(value):
    high = value.astype(BF16)
    low = (value - high.astype(F32)).astype(BF16)
    return high, low


def dot(a, b):
    return jnp.dot(a, b, preferred_element_type=F32)


def padded_k(matrices):
    rounded = lax.reduce_precision(matrices, 8, 7)
    low = matrices - rounded
    total = jnp.zeros((matrices.shape[0], 3 * HALF), F32)
    for part, value in enumerate((rounded, rounded, low)):
        after = 3 * HALF - part * HALF - matrices.shape[1]
        total = total + jnp.pad(value, ((0, 0), (part * HALF, after)))
    return total.astype(BF16)


def stack_columns(field, rhs_ref):
    basis = field.shape[0]
    high, low = two_parts(field)
    rhs_ref[0:basis, :] = high
    rhs_ref[HALF : HALF + basis, :] = low
    rhs_ref[2 * HALF : 2 * HALF + basis, :] = high


def clear_fill(rhs_ref, basis):
    for part in range(3):
        rhs_ref[part * HALF + basis : (part + 1) * HALF, :] = jnp.zeros(
            (HALF - basis, rhs_ref.shape[1]), BF16
        )


def pick_parts(high, low, chosen):
    width = high.shape[1]
    body = width - LANES
    ends = jnp.concatenate([high[:, body:], low[:, body:]], 1)
    return dot(high[:, :body], chosen[:body]) + dot(low[:, :body], chosen[:body]) + dot(ends, chosen[body:])


def pick(field, chosen):
    high, low = two_parts(field)
    if chosen.shape[0] > field.shape[1]:
        return pick_parts(high, low, chosen)
    return dot(high, chosen) + dot(low, chosen)


def apply_maps(unit, matrices, base, emit, quantities, basis, unroll):
    group = 3
    tile, part = unit // group, unit % group
    lanes = pl.ds(pl.multiple_of(tile * LANES, LANES), LANES)

    def column(q, total):
        total = list(total)
        rows = pl.ds(pl.multiple_of(q * basis, 8), basis)
        for ref, at, sign, terms_ref, slot in matrices:
            term = terms_ref[slot, rows, lanes]
            for k in range(group):
                product = ref[group * part + k, q, at : at + 1, lanes] * term
                total[k] = total[k] + product if sign > 0 else total[k] - product
        return tuple(total)

    def rows_of(k):
        return pl.ds(pl.multiple_of((group * part + k) * basis, 8), basis)

    total = tuple(base(rows_of(k), lanes) for k in range(group))
    if unroll:
        for q in range(quantities):
            total = column(q, total)
    else:
        total = lax.fori_loop(0, quantities, column, total)
    for k in range(group):
        emit(rows_of(k), lanes, total[k])


def apply_tile(tile, matrices, base, emit, quantities, basis):
    lanes = pl.ds(pl.multiple_of(tile * LANES, LANES), LANES)
    group = 3
    for first in range(0, quantities, group):

        def column(q, total):
            total = list(total)
            rows = pl.ds(pl.multiple_of(q * basis, 8), basis)
            for ref, at, sign, terms_ref, slot in matrices:
                term = terms_ref[slot, rows, lanes]
                for k in range(group):
                    product = ref[first + k, q, at : at + 1, lanes] * term
                    total[k] = total[k] + product if sign > 0 else total[k] - product
            return tuple(total)

        start = tuple(base(first + k, lanes) for k in range(group))
        total = lax.fori_loop(0, quantities, column, start)
        for k in range(group):
            emit(first + k, lanes, total[k])


def pack(field, select_ref, weight_ref, message_refs, values_ref, quantities, basis):
    rows = quantities * basis
    lane = lax.broadcasted_iota(jnp.int32, (SEND_ROWS, LANES), 1) < HALF
    tail = SEND_ROWS - (rows - SEND_ROWS)
    pairs = len(message_refs) // 2
    if values_ref is None:
        picked = pick(field, select_ref[:, : pairs * LANES])
    elif not pairs:
        picked = pick(field, select_ref[:, select_ref.shape[1] - LANES :])
    else:
        picked = pick(field, select_ref[...])
    for pair in range(pairs):
        block = picked[:, pair * LANES : (pair + 1) * LANES]
        top = block[:SEND_ROWS]
        bottom = jnp.concatenate([block[SEND_ROWS:], jnp.zeros((tail, LANES), F32)], 0)
        message_refs[2 * pair][...] = jnp.where(lane, top, pltpu.roll(bottom, HALF, 1))
        message_refs[2 * pair + 1][...] = jnp.where(lane, pltpu.roll(top, HALF, 1), bottom)
    if values_ref is None:
        return
    receivers = weight_ref.shape[1]
    block = picked[:, pairs * LANES : pairs * LANES + receivers]
    for q in range(quantities):
        values_ref[q : q + 1, :] = jnp.sum(
            block[q * basis : (q + 1) * basis] * weight_ref[...], axis=0, keepdims=True
        )


def first_kernel(quantities, count_ref, field_ref, send_ref, receiver_ref, select_ref, *messages):
    rows = field_ref.shape[0]
    width = select_ref.shape[0]
    slots, capacity = send_ref.shape
    receivers = receiver_ref.shape[1]
    select_ref[:, slots * capacity :] = jnp.zeros((width, LANES), BF16)
    element = lax.broadcasted_iota(jnp.int32, (width, capacity), 0)
    element = jnp.where(element < field_ref.shape[1], element, element - LANES)
    place = lax.broadcasted_iota(jnp.int32, (1, capacity), 1)
    for slot in range(slots):
        asked = jnp.where(place < count_ref[0, slot], send_ref[slot : slot + 1, :], -1)
        select_ref[:, slot * capacity : (slot + 1) * capacity] = jnp.where(
            element == asked, 1.0, 0.0
        ).astype(BF16)
    element = lax.broadcasted_iota(jnp.int32, (width, receivers), 0)
    element = jnp.where(element < field_ref.shape[1], element, element - LANES)
    select_ref[:, slots * capacity : slots * capacity + receivers] = jnp.where(
        element == receiver_ref[...], 1.0, 0.0
    ).astype(BF16)
    pack(field_ref[...], select_ref, None, messages, None, quantities, rows // quantities)


def own_maps(star_ref, local_ref, terms_ref):
    stars = star_ref.shape[2]
    return [(star_ref, n, 1, terms_ref, n) for n in range(stars)] + [
        (local_ref, f, -1, terms_ref, stars + f) for f in range(local_ref.shape[2])
    ]


def own_kernel_a(field_ref, matrix_ref, star_ref, local_ref, terms_ref, high_ref, low_ref, out_ref, rhs_ref, flux_ref):
    faces = high_ref.shape[0]
    locals_, rows_all, width = terms_ref.shape
    basis = matrix_ref.shape[0] // (locals_ + faces)
    quantities = rows_all // basis
    clear_fill(rhs_ref, basis)

    def modal(first, count):
        for k in range(count):
            rows = pl.ds(pl.multiple_of((first + k) * basis, 8), basis)
            stack_columns(field_ref[rows, :], rhs_ref.at[:, k * width : (k + 1) * width])
        for at in range(0, count * width, 2 * LANES):
            end = min(at + 2 * LANES, count * width)
            result = dot(matrix_ref[...], rhs_ref[:, at:end])
            for low in range(at, end, LANES):
                k, lane = low // width, low % width
                rows = pl.ds(pl.multiple_of((first + k) * basis, 8), basis)
                for n in range(locals_ + faces):
                    value = result[n * basis : (n + 1) * basis, low - at : low - at + LANES]
                    if n < locals_:
                        terms_ref[n, rows, lane : lane + LANES] = value
                    else:
                        flux_ref[n - locals_, rows, lane : lane + LANES] = value

    def pair(i, carry):
        modal(2 * i, 2)
        return carry

    lax.fori_loop(0, quantities // 2, pair, 0)
    if quantities % 2:
        modal(quantities - 1, 1)

    def parts(f, carry):
        high_ref[f], low_ref[f] = two_parts(flux_ref[f])
        return carry

    lax.fori_loop(0, faces, parts, 0)

    def base(rows, lanes):
        return field_ref[rows, lanes]

    def emit(rows, lanes, value):
        out_ref[rows, :] = value

    def plain(unit, carry):
        apply_maps(unit, own_maps(star_ref, local_ref, terms_ref), base, emit, quantities, basis, False)
        return carry

    units = 3 * width // LANES
    lax.fori_loop(units - 3, units, plain, 0)


def own_kernel_b(field_ref, terms_ref, star_ref, local_ref, high_ref, low_ref, choose_ref, out_ref, gathered_ref):
    quantities = star_ref.shape[0]
    basis = field_ref.shape[0] // quantities

    def base(rows, lanes):
        return field_ref[rows, lanes]

    def emit(rows, lanes, value):
        out_ref[rows, lanes] = value

    def face(f, carry):
        gathered_ref[f] = pick_parts(high_ref[f], low_ref[f], choose_ref[f])
        for k in range(3):
            apply_maps(3 * f + k, own_maps(star_ref, local_ref, terms_ref), base, emit, quantities, basis, True)
        return carry

    lax.fori_loop(0, high_ref.shape[0], face, 0)


def halo_kernel(slots, sends, live_ref, field_ref, partial_ref, partial_b_ref, gathered_ref, matrix_ref, remote_ref, choose_ref, energy_ref, select_ref, weight_ref, *rest):
    halo_refs = rest[:slots]
    state_ref, power_ref, values_ref = rest[slots : slots + 3]
    messages = rest[slots + 3 : slots + 3 + sends]
    columns_ref, flux_ref, terms_ref, rhs_ref = rest[slots + 3 + sends :]
    quantities, _, faces = remote_ref.shape[:3]
    rows_all, width = field_ref.shape
    basis = rows_all // quantities
    clear_fill(rhs_ref, basis)
    lane = lax.broadcasted_iota(jnp.int32, (SEND_ROWS, LANES), 1) < HALF
    for pair in range(slots // 2):
        a = halo_refs[2 * pair][...]
        b = halo_refs[2 * pair + 1][...]
        lanes = slice(pair * LANES, (pair + 1) * LANES)
        columns_ref[0:SEND_ROWS, lanes] = jnp.where(lane, a, pltpu.roll(b, HALF, 1))
        bottom = jnp.where(lane, pltpu.roll(a, HALF, 1), b)
        columns_ref[SEND_ROWS:, lanes] = bottom[: rows_all - SEND_ROWS]

    def modal(q, carry):
        rows = pl.ds(pl.multiple_of(q * basis, 8), basis)
        stack_columns(columns_ref[rows, :], rhs_ref)
        result = dot(matrix_ref[...], rhs_ref[...])
        for f in range(faces):
            flux_ref[f, rows, :] = result[f * basis : (f + 1) * basis]
        return carry

    lax.fori_loop(0, quantities, modal, 0)

    def gather(f, carry):
        terms_ref[f] = gathered_ref[f] + pick(flux_ref[f], choose_ref[f])
        return carry

    lax.fori_loop(0, faces, gather, 0)
    matrices = [(remote_ref, f, -1, terms_ref, f) for f in range(faces)]

    def tile_body(partial_ref, first, tile, power):
        totals = [power]
        own = pl.ds(pl.multiple_of((tile - first) * LANES, LANES), LANES)

        def base(p, lanes):
            return partial_ref[p * basis : (p + 1) * basis, own]

        def emit(p, lanes, value):
            live = live_ref[0:1, lanes] > 0
            kept = jnp.where(live, value, field_ref[p * basis : (p + 1) * basis, lanes])
            state_ref[p * basis : (p + 1) * basis, lanes] = kept
            squares = kept * kept * energy_ref[p : p + 1, lanes]
            for block in range(basis // 8):
                totals[0] = totals[0] + squares[block * 8 : (block + 1) * 8]

        apply_tile(tile, matrices, base, emit, quantities, basis)
        return totals[0]

    tiles = width // LANES
    power = jnp.zeros((8, LANES), F32)
    power = lax.fori_loop(0, tiles - 1, lambda tile, power: tile_body(partial_ref, 0, tile, power), power)
    power_ref[...] = tile_body(partial_b_ref, tiles - 1, tiles - 1, power)
    pack(state_ref[...], select_ref, weight_ref, messages, values_ref, quantities, basis)


def vmem(count):
    return [pl.BlockSpec(memory_space=pltpu.VMEM)] * count


def smem(count):
    return [pl.BlockSpec(memory_space=pltpu.SMEM)] * count


def granted(mib, flops=0):
    extra = {}
    if flops:
        extra["cost_estimate"] = pl.CostEstimate(flops=flops, bytes_accessed=8_000_000, transcendentals=0)
    return dict(compiler_params=pltpu.CompilerParams(vmem_limit_bytes=mib * 2**20), **extra)


def per_device(
    element_state,
    stiffness,
    flux_local,
    flux_remote,
    star_matrix,
    face_local,
    face_remote,
    energy_weight,
    face_neighbour,
    element_count,
    send_count,
    send_element,
    receiver_element,
    receiver_slot,
    receiver_weight,
):
    basis, quantities, width = element_state.shape
    slots, capacity = send_element.shape[1:]
    faces = face_neighbour.shape[0]
    receivers = receiver_slot.shape[0]
    group_size = lax.axis_size("dom")
    rows = basis * quantities
    locals_ = stiffness.shape[0] + faces
    halo_width = slots * capacity

    fields = element_state.transpose(1, 0, 2).reshape(rows, width)
    star = star_matrix.transpose(1, 2, 0, 3)
    local = face_local.transpose(1, 2, 0, 3)
    remote = face_remote.transpose(1, 2, 0, 3)

    message = jax.ShapeDtypeStruct((SEND_ROWS, LANES), F32)
    values_shape = jax.ShapeDtypeStruct((quantities, receivers), F32)
    field_shape = jax.ShapeDtypeStruct((rows, width), F32)
    power_shape = jax.ShapeDtypeStruct((8, LANES), F32)
    terms_shape = jax.ShapeDtypeStruct((locals_, rows, width), F32)
    parts_shape = jax.ShapeDtypeStruct((faces, rows, width), BF16)
    gathered_shape = jax.ShapeDtypeStruct((faces, rows, width), F32)
    select_shape = jax.ShapeDtypeStruct((width + LANES, halo_width + LANES), BF16)
    outs = pl.pallas_call(
        lambda *refs: first_kernel(quantities, *refs),
        out_shape=(select_shape,) + (message,) * slots,
        in_specs=smem(1) + vmem(3),
        out_specs=tuple(vmem(slots + 1)),
        name="first_messages",
        **granted(16),
    )(send_count, fields, send_element[0], receiver_element[None, :])
    select, messages = outs[0], outs[1:]

    element_row = jnp.arange(width + LANES, dtype=jnp.int32)[:, None]
    element_row = jnp.where(element_row < width, element_row, element_row - LANES)
    choose_own = (element_row[None] == face_neighbour[:, None, :]).astype(BF16)
    halo_row = jnp.arange(halo_width, dtype=jnp.int32)[:, None] + width
    choose_halo = (halo_row[None] == face_neighbour[:, None, :]).astype(BF16)
    own_matrix = padded_k(jnp.concatenate([stiffness, flux_local, flux_remote], 0).reshape(-1, basis))
    halo_matrix = own_matrix[locals_ * basis :]

    live = (jnp.arange(width, dtype=jnp.int32) < element_count[0]).astype(F32)[None, :]
    live_energy = jnp.where(live > 0, energy_weight, 0.0)

    def send(slot, value):
        if slot < 2 * PEER_REACH:
            offset = slot + 1 if slot < PEER_REACH else PEER_REACH - 1 - slot
            pairs = [(i, (i + offset) % group_size) for i in range(group_size)]
            return lax.ppermute(value, "dom", pairs)
        offset = 1 if slot == 2 * PEER_REACH else -1
        count = lax.axis_size("grp")
        pairs = [(i, i + offset) for i in range(count) if 0 <= i + offset < count]
        return lax.ppermute(value, "grp", pairs)

    powers = []
    samples = []
    for step in range(TIME_STEPS):
        last = step == TIME_STEPS - 1
        arrived = [None] * slots
        for slot in FIRST_SENDS:
            arrived[slot] = send(slot, messages[slot])
        terms, high, low, partial_b = pl.pallas_call(
            own_kernel_a,
            out_shape=(terms_shape, parts_shape, parts_shape, jax.ShapeDtypeStruct((rows, LANES), F32)),
            in_specs=vmem(4),
            out_specs=tuple(vmem(4)),
            scratch_shapes=[pltpu.VMEM((3 * HALF, 2 * width), BF16), pltpu.VMEM((faces, rows, width), F32)],
            name="own_terms_a",
            **granted(10, 5_000_000_000),
        )(fields, own_matrix, star, local)
        others = [slot for slot in range(slots) if slot not in FIRST_SENDS]
        held = lax.optimization_barrier(tuple(messages[slot] for slot in others) + (partial_b,))
        partial_b = held[-1]
        for slot, value in zip(others, held):
            arrived[slot] = send(slot, value)
        partial, gathered = pl.pallas_call(
            own_kernel_b,
            out_shape=(jax.ShapeDtypeStruct((rows, width - LANES), F32), gathered_shape),
            in_specs=vmem(7),
            out_specs=tuple(vmem(2)),
            name="own_terms_b",
            **granted(6, 5_000_000_000),
        )(fields, terms, star, local, high, low, choose_own)
        sends = 0 if last else slots
        outs = pl.pallas_call(
            lambda *refs, sends=sends: halo_kernel(slots, sends, *refs),
            out_shape=(field_shape, power_shape, values_shape) + (message,) * sends,
            in_specs=vmem(11 + slots),
            out_specs=tuple(vmem(3 + sends)),
            scratch_shapes=[
                pltpu.VMEM((rows, halo_width), F32),
                pltpu.VMEM((faces, rows, halo_width), F32),
                pltpu.VMEM((faces, rows, width), F32),
                pltpu.VMEM((3 * HALF, halo_width), BF16),
            ],
            name="halo_terms_last" if last else "halo_terms",
            **granted(18, 6_000_000_000),
        )(live, fields, partial, partial_b, gathered, halo_matrix, remote, choose_halo, live_energy, select, receiver_weight, *arrived)
        fields, messages = outs[0], outs[3:]
        powers.append(outs[1])
        samples.append(outs[2])

    new_state = fields.reshape(quantities, basis, width).transpose(1, 0, 2)
    denominator = float(group_size * width * basis * quantities)
    own_energy = 0.5 * jnp.sum(jnp.stack(powers), axis=(1, 2))
    values = jnp.concatenate(samples, 0)
    matches = (receiver_slot[:, None] == jnp.arange(group_size * receivers)[None, :]).astype(F32)
    placed = jnp.dot(values, matches, precision=highest, preferred_element_type=F32)
    pieces = placed.reshape(-1, group_size, receivers).transpose(1, 0, 2).reshape(group_size, -1)
    fill = jnp.zeros((group_size, 16 - TIME_STEPS), F32)
    spread = jnp.broadcast_to(own_energy[None, :], (group_size, TIME_STEPS))
    pieces = jnp.concatenate([pieces, spread, fill], 1)
    arrived = lax.all_to_all(pieces, "dom", split_axis=0, concat_axis=0, tiled=True)
    total = arrived.sum(axis=0)
    traces = total[: TIME_STEPS * quantities * receivers].reshape(TIME_STEPS, quantities, receivers)
    energy = total[TIME_STEPS * quantities * receivers :][:TIME_STEPS] / denominator
    return (new_state, energy[None, :], traces)


def solution(mesh):
    return jax.shard_map(
        per_device,
        mesh=mesh,
        in_specs=(
            P(None, None, GRP_DOM),
            P(),
            P(),
            P(),
            P(None, None, None, GRP_DOM),
            P(None, None, None, GRP_DOM),
            P(None, None, None, GRP_DOM),
            P(None, GRP_DOM),
            P(None, GRP_DOM),
            P(GRP_DOM),
            P(GRP_DOM, None),
            P(GRP_DOM, None, None),
            P(GRP_DOM),
            P(GRP_DOM),
            P(None, GRP_DOM),
        ),
        out_specs=(P(None, None, GRP_DOM), P("grp", None), P(None, None, GRP_DOM)),
        check_vma=False,
    )
```
